32 devices in a mesh: parts: 2 (over y), samp: 16 (over z, x, core).
Axes of the slice: x: 2, y: 2, z: 4, core: 2. Of those that a mesh axis runs over, the one named last changes fastest.
Arguments:
- expression: bfloat16 [1024, 20480], P(('parts', 'samp')), parts along dimension 0, may hold values from -6 to 6
- current: bfloat16 [1024, 256], P(('parts', 'samp')), parts along dimension 0, may hold values from -6 to 6
- next_packed: int32 [512, 32], P(('parts', 'samp')), parts along dimension 0, may hold values from -2147483648 to 1789569706, as said below
- covariates: float32 [1024, 64], P(('parts', 'samp')), parts along dimension 0, may hold values from -1 to 1
Outputs:
- scores: float32 [40960, 256], P(('parts', 'samp')), parts along dimension 0
- next_block: bfloat16 [1024, 256], P(('parts', 'samp')), parts along dimension 0
The draws below stay inside these ranges and needn't reach their ends.
There are 2 independent parts, one for each index of `parts`. The reference program is written for one: setup_inputs(seed, part) draws one part's arguments, and reference() takes and returns one part's arrays. A program takes and returns all parts, laid end to end along the dimension named above; each array names one. Nothing has to cross between parts.
Inputs may be any that keep to these rules, and one draw needn't show every extreme that they name: Each word holds the dosages (0, 1 or 2) of 16 consecutive samples of one variant, two bits a sample: sample 16 w + j of variant v in bits 2 j and 2 j + 1 of next_packed[v, w], bit 31 being the sign bit of the int32 word.
All inputs are finite; a program needn't handle non-finite values.
Results may differ from the reference program's by a relative error of at most 0.0004.
Values may be sent and summed in bfloat16 or wider, within the bound.
A program may use at most 64 MiB of HBM per device.

```python
import jax
import jax.numpy as jnp
from jax import lax

GENES = 20480
VARS = 256
COVS = 64
SAMPLES = 512


def draw_next_packed(key, part):
    base = jax.random.fold_in(key, 11)
    key_freq, key_first, key_second = jax.random.split(base, 3)
    word_count = SAMPLES // 16
    allele = jax.random.randint(key_freq, (VARS, 1, 1), 200, 1001, dtype=jnp.int32)
    sample_index = 16 * jnp.arange(word_count, dtype=jnp.int32)[None, :, None] + jnp.arange(16, dtype=jnp.int32)[None, None, :]
    thresh = allele * (100 + 400 * sample_index // SAMPLES) // 1000
    first = jax.random.randint(key_first, (VARS, word_count, 16), 0, 1000, dtype=jnp.int32)
    second = jax.random.randint(key_second, (VARS, word_count, 16), 0, 1000, dtype=jnp.int32)
    dose = (first < thresh).astype(jnp.int32) + (second < thresh).astype(jnp.int32)
    shifts = 2 * jnp.arange(16, dtype=jnp.int32)
    return jnp.sum(lax.shift_left(dose, shifts[None, None, :]), axis=2, dtype=jnp.int32)


def draw_covariates(key, part):
    base = jax.random.fold_in(key, 7)
    key_noise, key_phase = jax.random.split(base, 2)
    noise = jax.random.normal(key_noise, (SAMPLES, COVS), jnp.float32)
    noise = noise * float(SAMPLES) ** (-0.5)
    phase = jax.random.uniform(key_phase, (COVS,), jnp.float32, 0.0, 6.2831853)
    column = jnp.arange(COVS, dtype=jnp.int32)
    freq = (column % 8 + 1).astype(jnp.float32)
    position = (jnp.arange(SAMPLES, dtype=jnp.float32) + 0.5) / SAMPLES
    smooth = jnp.cos(3.14159265 * freq[None, :] * position[:, None] + phase[None, :]) * (2.0 / SAMPLES) ** 0.5
    return jnp.where((column < 8)[None, :], 0.5 * noise + 0.85 * smooth, noise)


def spiked(result, stream_key, source, target, blocks, factor):
    owner, partner = [(jnp.arange(result.shape[dim]) // (result.shape[dim] // blocks)).reshape([-1 if axis == dim else 1 for axis in range(result.ndim)]) for dim in (source, target)]
    chosen = jax.random.permutation(stream_key, blocks)[partner]
    strong = (owner == chosen) | (owner == (partner + blocks // 2) % blocks)
    return jnp.where(strong, factor * result, result)


def block_scale(stream_key, extent, cuts, low, largest):
    level, own = 1.0, jax.random.fold_in(stream_key, 6)
    for dim, parts in cuts:
        draws = jnp.exp(jax.random.uniform(jax.random.fold_in(own, dim), (parts,), jnp.float32, low / len(cuts), largest / len(cuts)))
        level = level * jnp.repeat(draws, extent[dim] // parts).reshape([-1 if axis == dim else 1 for axis in range(len(extent))])
    return level


def scatter_about(rng, dims, spread, most, pieces=(), kind=jnp.bfloat16):
    loudness = block_scale(rng, dims, pieces, -0.22, 0.18) if pieces else 1.0
    result = jax.random.normal(rng, dims, jnp.float32) * spread * loudness
    return jnp.minimum(jnp.maximum(result, -most), most).astype(kind)


def bell_draw_with(stream_key, dims, deviation, limit, cuts, heavy, held_as=jnp.bfloat16):
    drawn = deviation * jax.random.normal(stream_key, dims, jnp.float32)
    if cuts:
        drawn = drawn * block_scale(stream_key, dims, cuts, -0.22, 0.18)
    return jnp.clip(spiked(drawn, jax.random.fold_in(stream_key, 3), *heavy), -limit, limit).astype(held_as)


def setup_inputs(seed: int = 0, part: int = 0) -> dict:
    seeds = jax.random.split(jax.random.key(seed), 5)
    own_keys = jax.random.split(jax.random.fold_in(seeds[4], part), 5)
    expression = bell_draw_with(own_keys[0], (SAMPLES, GENES), 1.0, 6.0, ((0, 16),), (0, 1, 16, 2.0))
    current = scatter_about(own_keys[1], (SAMPLES, VARS), 1.0, 6.0, ((0, 16),))
    next_packed = draw_next_packed(jax.random.fold_in(jax.random.fold_in(seeds[4], part), 71), part)
    covariates = draw_covariates(jax.random.fold_in(jax.random.fold_in(seeds[4], part), 71), part)
    return dict(expression=expression, current=current, next_packed=next_packed, covariates=covariates)


def unpack_words(packed_words):
    shifts = 2 * jnp.arange(16, dtype=jnp.int32)
    fields = jnp.bitwise_and(lax.shift_right_logical(packed_words[:, :, None], shifts[None, None, :]), 3)
    return fields.reshape(packed_words.shape[0], -1).T.astype(jnp.float32)

def reference(expression, current, next_packed, covariates):
    scale_factor = float(SAMPLES) ** (-0.5)
    scores = lax.dot_general(expression, current, (((0,), (0,)), ((), ())), preferred_element_type=jnp.float32) * scale_factor
    dosage = unpack_words(next_packed)
    average = lax.optimization_barrier(jnp.sum(dosage, axis=0)) / SAMPLES
    projected = lax.dot_general(covariates, dosage, (((0,), (0,)), ((), ())), precision=lax.Precision.HIGHEST)
    cov_sums = lax.optimization_barrier(jnp.sum(covariates, axis=0))
    loading = projected - cov_sums[:, None] * average[None, :]
    leftover = dosage - average[None, :] - jnp.dot(covariates, loading, precision=lax.Precision.HIGHEST)
    sq_norm = lax.optimization_barrier(jnp.sum(leftover * leftover, axis=0))
    next_block = (leftover * lax.rsqrt(sq_norm / SAMPLES + 1e-05)[None, :]).astype(jnp.bfloat16)
    return (scores, next_block)
```

```python
import functools

import jax
import jax.numpy as jnp
from jax import lax
from jax.experimental import pallas as pl
from jax.experimental.pallas import tpu as pltpu
from jax.sharding import PartitionSpec as P

MESH = pl.DeviceIdType.MESH
CORES = 2


def unpack_words(packed_words):
    shifts = 2 * jnp.arange(16, dtype=jnp.int32)
    fields = jnp.bitwise_and(
        lax.shift_right_logical(packed_words[:, :, None], shifts[None, None, :]), 3
    )
    return fields.reshape(packed_words.shape[0], -1).T.astype(jnp.float32)


def over_samples(left, right):
    return lax.dot_general(
        left, right, (((0,), (0,)), ((), ())), preferred_element_type=jnp.float32
    )


def precise_samples(left, right):
    return lax.dot_general(left, right, (((0,), (0,)), ((), ())), precision=lax.Precision.HIGHEST)


def grid_of(group_size):
    chips = group_size // CORES
    across = 2 ** ((chips.bit_length() - 1) // 3)
    return chips // across, across


def exchange_kernel(
    depth,
    across,
    genes,
    expr_ref,
    current_ref,
    packed_ref,
    cov_ref,
    tiles_ref,
    current_all,
    next_ref,
    cov_all,
    packed_all,
    dosage_ref,
    words_ref,
    own_sem,
    bulk_send,
    bulk_recv,
    small_send,
    small_recv,
):
    me = lax.axis_index("samp")
    core = lax.rem(me, CORES)
    column = lax.rem(me // CORES, across)
    level = me // (CORES * across)
    group_size = CORES * across * depth
    rows = cov_ref.shape[0]
    inward = jnp.where(level < depth // 2, 1, depth - 1)

    def member(dz, dx, dc):
        z = lax.rem(level + inward * dz, depth)
        x = lax.rem(column + dx, across)
        c = lax.rem(core + dc, CORES)
        return (z * across + x) * CORES + c

    barrier = pltpu.get_barrier_semaphore()
    for step in range(1, group_size):
        pl.semaphore_signal(
            barrier,
            inc=1,
            device_id={"samp": lax.rem(me + step, group_size)},
            device_id_type=MESH,
        )
    pl.semaphore_wait(barrier, group_size - 1)

    small = ((current_ref, current_all), (packed_ref, packed_all), (cov_ref, cov_all))
    own_copies = []
    for k, (own, whole) in enumerate(small):
        own_copies.append(
            pltpu.make_async_copy(own, whole.at[level, column, core], own_sem.at[k])
        )
    mine = pl.ds(pl.multiple_of(me * genes, 128), genes)
    own_copies.append(
        pltpu.make_async_copy(expr_ref.at[:, mine], tiles_ref.at[me], own_sem.at[len(small)])
    )
    for copy in own_copies:
        copy.start()

    def small_along_z(k, dz, sender_level):
        own, whole = small[k]
        target = (lax.rem(level + dz, depth) * across + column) * CORES + core
        return pltpu.make_async_remote_copy(
            src_ref=own,
            dst_ref=whole.at[sender_level, column, core],
            send_sem=small_send.at[k, dz],
            recv_sem=small_recv.at[k, dz],
            device_id={"samp": target},
            device_id_type=MESH,
        )

    def bulk(other, sender):
        span = pl.ds(pl.multiple_of(other * genes, 128), genes)
        return pltpu.make_async_remote_copy(
            src_ref=expr_ref.at[:, span],
            dst_ref=tiles_ref.at[sender],
            send_sem=bulk_send.at[other],
            recv_sem=bulk_recv.at[sender],
            device_id={"samp": other},
            device_id_type=MESH,
        )

    for dz in range(1, depth):
        for k in range(len(small)):
            small_along_z(k, dz, level).start()
    same_column = [(dz, 0, dc) for dz in range(1, depth) for dc in range(CORES)]
    others = [
        (dz, dx, dc)
        for dz in [*range(1, depth), 0]
        for dx in range(1, across)
        for dc in range(CORES)
    ]
    for offset in same_column:
        bulk(member(*offset), me).start()
    for copy in own_copies[: len(small)]:
        copy.wait()
    for dz in range(1, depth):
        for k in range(len(small)):
            small_along_z(k, dz, lax.rem(level - dz + depth, depth)).wait_recv()

    def small_along_x(k, dx, sender_column):
        whole = small[k][1]
        target = (level * across + lax.rem(column + dx, across)) * CORES + core
        return pltpu.make_async_remote_copy(
            src_ref=whole.at[:, column, core],
            dst_ref=whole.at[:, sender_column, core],
            send_sem=small_send.at[k, depth + dx],
            recv_sem=small_recv.at[k, depth + dx],
            device_id={"samp": target},
            device_id_type=MESH,
        )

    for dx in range(1, across):
        for k in range(len(small)):
            small_along_x(k, dx, column).start()
    for offset in others:
        bulk(member(*offset), me).start()
    bulk(member(0, 0, 1), me).start()
    for dx in range(1, across):
        for k in range(len(small)):
            small_along_x(k, dx, lax.rem(column - dx + across, across)).wait_recv()

    def small_to_core(k, sender_core):
        whole = small[k][1]
        return pltpu.make_async_remote_copy(
            src_ref=whole.at[:, :, core],
            dst_ref=whole.at[:, :, sender_core],
            send_sem=small_send.at[k, 0],
            recv_sem=small_recv.at[k, 0],
            device_id={"samp": me - core + (1 - core)},
            device_id_type=MESH,
        )

    for k in range(len(small)):
        small_to_core(k, core).start()
    for k in range(len(small)):
        small_to_core(k, 1 - core).wait_recv()

    samples = group_size * rows
    variants = group_size * packed_ref.shape[0]
    word_count = packed_ref.shape[1]
    words_ref[...] = packed_all[...].reshape(variants, word_count).T
    shifts = 2 * lax.broadcasted_iota(jnp.int32, (16, variants), 0)

    @pl.loop(0, word_count)
    def _(word):
        held = jnp.broadcast_to(words_ref[pl.ds(word, 1), :], (16, variants))
        fields = jnp.bitwise_and(lax.shift_right_logical(held, shifts), 3)
        dosage_ref[pl.ds(pl.multiple_of(word * 16, 16), 16), :] = fields.astype(jnp.float32)

    cov = cov_all[...].reshape(samples, cov_ref.shape[1])
    average = jnp.sum(dosage_ref[...], axis=0, keepdims=True) / samples
    projected = precise_samples(cov, dosage_ref[...])
    cov_sums = precise_samples(cov, jnp.ones((samples, 128), jnp.float32))[:, :1]
    loading = projected - cov_sums * average
    leftover = (
        dosage_ref[...]
        - average
        - jnp.dot(cov, loading, precision=lax.Precision.HIGHEST, preferred_element_type=jnp.float32)
    )
    sq_norm = jnp.sum(leftover * leftover, axis=0, keepdims=True)
    dosage_ref[...] = leftover
    here = dosage_ref[pl.ds(pl.multiple_of(me * rows, 8), rows), :]
    next_ref[...] = (here * lax.rsqrt(sq_norm / samples + 1e-05)).astype(next_ref.dtype)

    own_copies[-1].wait()
    for offset in [*same_column, *others, (0, 0, 1)]:
        other = member(*offset)
        bulk(other, me).wait_send()
    for step in range(1, group_size):
        bulk(me, lax.rem(me + step, group_size)).wait_recv()
    for k in range(len(small)):
        for dz in range(1, depth):
            small_along_z(k, dz, level).wait_send()
        for dx in range(1, across):
            small_along_x(k, dx, column).wait_send()
        small_to_core(k, core).wait_send()


def exchange(expression, current, next_packed, covariates, group_size):
    depth, across = grid_of(group_size)
    rows, all_genes = expression.shape
    genes = all_genes // group_size
    variants = next_packed.shape[0] * group_size
    lead = (depth, across, CORES)
    vmem = pl.BlockSpec(memory_space=pltpu.VMEM)
    hbm = pl.BlockSpec(memory_space=pl.ANY)
    return pl.pallas_call(
        functools.partial(exchange_kernel, depth, across, genes),
        out_shape=(
            jax.ShapeDtypeStruct((group_size, rows, genes), expression.dtype),
            jax.ShapeDtypeStruct((*lead, *current.shape), current.dtype),
            jax.ShapeDtypeStruct(current.shape, jnp.bfloat16),
        ),
        in_specs=[hbm, vmem, vmem, vmem],
        out_specs=(hbm, vmem, vmem),
        scratch_shapes=[
            pltpu.VMEM((*lead, *covariates.shape), covariates.dtype),
            pltpu.VMEM((*lead, *next_packed.shape), next_packed.dtype),
            pltpu.VMEM((rows * group_size, variants), jnp.float32),
            pltpu.VMEM((next_packed.shape[1], variants), jnp.int32),
            pltpu.SemaphoreType.DMA((4,)),
            pltpu.SemaphoreType.DMA((group_size,)),
            pltpu.SemaphoreType.DMA((group_size,)),
            pltpu.SemaphoreType.DMA((3, depth + across)),
            pltpu.SemaphoreType.DMA((3, depth + across)),
        ],
        compiler_params=pltpu.CompilerParams(collective_id=0, has_side_effects=True),
    )(expression, current, next_packed, covariates)


def shards(expression, current, next_packed, covariates):
    group_size = lax.axis_size("samp")
    samples_all = expression.shape[0] * group_size
    scale_factor = float(samples_all) ** (-0.5)
    genes = expression.shape[1] // group_size
    if genes % 128 == 0 and next_packed.shape[0] % 8 == 0:
        tiles, current_all, next_block = exchange(
            expression, current, next_packed, covariates, group_size
        )
        regrouped = tiles.reshape(samples_all, genes)
        everyone = current_all.reshape(samples_all, current.shape[1])
        return (over_samples(regrouped, everyone) * scale_factor, next_block)
    return shards_by_xla(expression, current, next_packed, covariates)


def shards_by_xla(expression, current, next_packed, covariates):
    group_size = lax.axis_size("samp")
    samples_all = expression.shape[0] * group_size
    scale_factor = float(samples_all) ** (-0.5)
    regrouped = lax.all_to_all(expression, "samp", split_axis=1, concat_axis=0, tiled=True)
    scores = (
        over_samples(regrouped, lax.all_gather(current, "samp", axis=0, tiled=True)) * scale_factor
    )
    packed_words = lax.all_to_all(next_packed, "samp", split_axis=1, concat_axis=0, tiled=True)
    dosage = unpack_words(packed_words)
    local_totals = jnp.sum(dosage, axis=0)
    local_proj = precise_samples(covariates, dosage)
    local_covsum = jnp.sum(covariates, axis=0)
    local_squares = jnp.sum(dosage * dosage, axis=0)
    local_gram = precise_samples(covariates, covariates)
    totals, projected, cov_sums, squares, cov_gram = lax.psum(
        (local_totals, local_proj, local_covsum, local_squares, local_gram), "samp"
    )
    average = totals / samples_all
    loading = projected - cov_sums[:, None] * average[None, :]
    leftover = (
        dosage - average[None, :] - jnp.dot(covariates, loading, precision=lax.Precision.HIGHEST)
    )
    mapped = jnp.dot(cov_gram, loading, precision=lax.Precision.HIGHEST)
    sq_norm = (
        squares
        - samples_all * average * average
        - 2.0 * jnp.sum(loading * loading, axis=0)
        + jnp.sum(loading * mapped, axis=0)
    )
    next_block = (leftover * lax.rsqrt(sq_norm / samples_all + 1e-05)[None, :]).astype(jnp.bfloat16)
    return (scores, next_block)


def solution(mesh):
    in_specs = (
        P(("parts", "samp"), None),
        P(("parts", "samp"), None),
        P(("parts", "samp"), None),
        P(("parts", "samp"), None),
    )
    out_specs = (P(("parts", "samp"), None), P(("parts", "samp"), None))
    return jax.shard_map(shards, mesh=mesh, in_specs=in_specs, out_specs=out_specs, check_vma=False)
```

```python
import functools

import jax
import jax.numpy as jnp
from jax import lax
from jax.experimental import pallas as pl
from jax.experimental.pallas import tpu as pltpu
from jax.sharding import PartitionSpec as P

MESH = pl.DeviceIdType.MESH
CORES = 2


def unpack_words(packed_words):
    shifts = 2 * jnp.arange(16, dtype=jnp.int32)
    fields = jnp.bitwise_and(
        lax.shift_right_logical(packed_words[:, :, None], shifts[None, None, :]), 3
    )
    return fields.reshape(packed_words.shape[0], -1).T.astype(jnp.float32)


def over_samples(left, right):
    return lax.dot_general(
        left, right, (((0,), (0,)), ((), ())), preferred_element_type=jnp.float32
    )


def precise_samples(left, right):
    return lax.dot_general(left, right, (((0,), (0,)), ((), ())), precision=lax.Precision.HIGHEST)


def grid_of(group_size):
    chips = group_size // CORES
    across = 2 ** ((chips.bit_length() - 1) // 3)
    return chips // across, across


def exchange_kernel(
    depth,
    across,
    genes,
    expr_ref,
    current_ref,
    packed_ref,
    cov_ref,
    tiles_ref,
    current_all,
    next_ref,
    cov_all,
    packed_all,
    dosage_ref,
    words_ref,
    own_sem,
    bulk_send,
    bulk_recv,
    small_send,
    small_recv,
    row_send,
    row_recv,
    ready_sem,
):
    me = lax.axis_index("samp")
    core = lax.rem(me, CORES)
    column = lax.rem(me // CORES, across)
    level = me // (CORES * across)
    group_size = CORES * across * depth
    rows = cov_ref.shape[0]
    last = depth - 1

    def at(z, x, c):
        return (z * across + x) * CORES + c

    def on_line(dz, act):
        z = level + dz
        pl.when(jnp.logical_and(z >= 0, z <= last))(functools.partial(act, z))

    row_mates = [
        (dx, dc) for dx in range(across) for dc in range(CORES) if (dx, dc) != (0, 0)
    ]

    def row_mate(z, dx, dc):
        return at(z, lax.rem(column + dx, across), lax.rem(core + dc, CORES))

    near_count = len(row_mates) + CORES * (
        jnp.where(level > 0, 1, 0) + jnp.where(level < last, 1, 0)
    )

    def greet(sem):
        def tell(target):
            pl.semaphore_signal(sem, inc=1, device_id={"samp": target}, device_id_type=MESH)

        def both_cores(z):
            for dc in range(CORES):
                tell(row_mate(z, 0, dc))

        on_line(1, both_cores)
        on_line(-1, both_cores)
        for dx, dc in row_mates:
            tell(row_mate(level, dx, dc))

    small = ((current_ref, current_all), (packed_ref, packed_all), (cov_ref, cov_all))

    def small_on_line(k, hop, step, source):
        own, whole = small[k]
        return pltpu.make_async_remote_copy(
            src_ref=own if hop == 0 else whole.at[source, column, core],
            dst_ref=whole.at[source, column, core],
            send_sem=small_send.at[k, hop * 2 + (step + 1) // 2],
            recv_sem=small_recv.at[k, source],
            device_id={"samp": at(level + step, column, core)},
            device_id_type=MESH,
        )

    def relay(hop, step, finish):
        source = level - hop * step
        goes = jnp.logical_and(
            jnp.logical_and(source >= 0, source <= last),
            jnp.logical_and(level + step >= 0, level + step <= last),
        )

        @pl.when(goes)
        def _():
            for k in range(len(small)):
                copy = small_on_line(k, hop, step, source)
                if finish:
                    copy.wait_send()
                else:
                    copy.start()

    def arrive(distance):
        def take(z):
            for k in range(len(small)):
                small_on_line(k, 1, 1, z).wait_recv()

        on_line(distance, take)
        on_line(-distance, take)

    def small_on_row(k, dx, sender_column):
        whole = small[k][1]
        return pltpu.make_async_remote_copy(
            src_ref=whole.at[:, column, core],
            dst_ref=whole.at[:, sender_column, core],
            send_sem=row_send.at[k, dx],
            recv_sem=row_recv.at[k, dx],
            device_id={"samp": at(level, lax.rem(column + dx, across), core)},
            device_id_type=MESH,
        )

    def small_to_core(k, sender_core):
        whole = small[k][1]
        return pltpu.make_async_remote_copy(
            src_ref=whole.at[:, :, core],
            dst_ref=whole.at[:, :, sender_core],
            send_sem=row_send.at[k, 0],
            recv_sem=row_recv.at[k, 0],
            device_id={"samp": at(level, column, 1 - core)},
            device_id_type=MESH,
        )

    def bulk(other, sender):
        span = pl.ds(pl.multiple_of(other * genes, 128), genes)
        return pltpu.make_async_remote_copy(
            src_ref=expr_ref.at[:, span],
            dst_ref=tiles_ref.at[sender],
            send_sem=bulk_send.at[other],
            recv_sem=bulk_recv.at[sender],
            device_id={"samp": other},
            device_id_type=MESH,
        )

    def send_tiles(dz, columns):
        def start(z):
            for dx in columns:
                for dc in range(CORES):
                    bulk(row_mate(z, dx, dc), me).start()

        on_line(dz, start)
        on_line(-dz, start)

    barrier = pltpu.get_barrier_semaphore()
    greet(barrier)
    own_copies = []
    for k, (own, whole) in enumerate(small):
        own_copies.append(
            pltpu.make_async_copy(own, whole.at[level, column, core], own_sem.at[k])
        )
    mine = pl.ds(pl.multiple_of(me * genes, 128), genes)
    own_copies.append(
        pltpu.make_async_copy(expr_ref.at[:, mine], tiles_ref.at[me], own_sem.at[len(small)])
    )
    for copy in own_copies:
        copy.start()
    pl.semaphore_wait(barrier, near_count)

    elsewhere = list(range(1, across))
    for hops in range(1, depth + 1):
        if hops < depth:
            greet(ready_sem.at[hops - 1])
        if hops == 1:
            relay(0, 1, False)
            relay(0, -1, False)
        if hops == 2:
            arrive(1)
            relay(1, 1, False)
            relay(1, -1, False)
        if hops < depth:
            send_tiles(hops, [0])
        if hops >= 2:
            send_tiles(hops - 1, elsewhere)
        if hops < depth:
            pl.semaphore_wait(ready_sem.at[hops - 1], near_count)
    for dx, dc in row_mates:
        bulk(row_mate(level, dx, dc), me).start()
    for distance in range(2, depth):
        arrive(distance)
        if distance < last:
            relay(distance, 1, False)
            relay(distance, -1, False)
    for copy in own_copies[: len(small)]:
        copy.wait()
    for dx in elsewhere:
        for k in range(len(small)):
            small_on_row(k, dx, column).start()
    for dx in elsewhere:
        for k in range(len(small)):
            small_on_row(k, dx, lax.rem(column - dx + across, across)).wait_recv()
    for k in range(len(small)):
        small_to_core(k, core).start()
    for k in range(len(small)):
        small_to_core(k, 1 - core).wait_recv()

    samples = group_size * rows
    variants = group_size * packed_ref.shape[0]
    word_count = packed_ref.shape[1]
    words_ref[...] = packed_all[...].reshape(variants, word_count).T
    shifts = 2 * lax.broadcasted_iota(jnp.int32, (16, variants), 0)

    @pl.loop(0, word_count)
    def _(word):
        held = jnp.broadcast_to(words_ref[pl.ds(word, 1), :], (16, variants))
        fields = jnp.bitwise_and(lax.shift_right_logical(held, shifts), 3)
        dosage_ref[pl.ds(pl.multiple_of(word * 16, 16), 16), :] = fields.astype(jnp.float32)

    cov = cov_all[...].reshape(samples, cov_ref.shape[1])
    average = jnp.sum(dosage_ref[...], axis=0, keepdims=True) / samples
    projected = precise_samples(cov, dosage_ref[...])
    cov_sums = precise_samples(cov, jnp.ones((samples, 128), jnp.float32))[:, :1]
    loading = projected - cov_sums * average
    leftover = (
        dosage_ref[...]
        - average
        - jnp.dot(cov, loading, precision=lax.Precision.HIGHEST, preferred_element_type=jnp.float32)
    )
    sq_norm = jnp.sum(leftover * leftover, axis=0, keepdims=True)
    dosage_ref[...] = leftover
    here = dosage_ref[pl.ds(pl.multiple_of(me * rows, 8), rows), :]
    next_ref[...] = (here * lax.rsqrt(sq_norm / samples + 1e-05)).astype(next_ref.dtype)

    own_copies[-1].wait()
    for step in range(1, group_size):
        bulk(lax.rem(me + step, group_size), me).wait_send()
    for step in range(1, group_size):
        bulk(me, lax.rem(me + step, group_size)).wait_recv()
    for hop in range(last):
        relay(hop, 1, True)
        relay(hop, -1, True)
    for k in range(len(small)):
        for dx in elsewhere:
            small_on_row(k, dx, column).wait_send()
        small_to_core(k, core).wait_send()


def exchange(expression, current, next_packed, covariates, group_size):
    depth, across = grid_of(group_size)
    rows, all_genes = expression.shape
    genes = all_genes // group_size
    variants = next_packed.shape[0] * group_size
    lead = (depth, across, CORES)
    vmem = pl.BlockSpec(memory_space=pltpu.VMEM)
    hbm = pl.BlockSpec(memory_space=pltpu.HBM)
    anywhere = pl.BlockSpec(memory_space=pl.ANY)
    return pl.pallas_call(
        functools.partial(exchange_kernel, depth, across, genes),
        out_shape=(
            jax.ShapeDtypeStruct((group_size, rows, genes), expression.dtype),
            jax.ShapeDtypeStruct((*lead, *current.shape), current.dtype),
            jax.ShapeDtypeStruct(current.shape, jnp.bfloat16),
        ),
        in_specs=[hbm] * 4,
        out_specs=(anywhere, vmem, vmem),
        scratch_shapes=[
            pltpu.VMEM((*lead, *covariates.shape), covariates.dtype),
            pltpu.VMEM((*lead, *next_packed.shape), next_packed.dtype),
            pltpu.VMEM((rows * group_size, variants), jnp.float32),
            pltpu.VMEM((next_packed.shape[1], variants), jnp.int32),
            pltpu.SemaphoreType.DMA((4,)),
            pltpu.SemaphoreType.DMA((group_size,)),
            pltpu.SemaphoreType.DMA((group_size,)),
            pltpu.SemaphoreType.DMA((3, 2 * depth)),
            pltpu.SemaphoreType.DMA((3, depth)),
            pltpu.SemaphoreType.DMA((3, across)),
            pltpu.SemaphoreType.DMA((3, across)),
            pltpu.SemaphoreType.REGULAR((depth,)),
        ],
        compiler_params=pltpu.CompilerParams(
            collective_id=0, has_side_effects=True
        ),
    )(expression, current, next_packed, covariates)


def shards(expression, current, next_packed, covariates):
    group_size = lax.axis_size("samp")
    samples_all = expression.shape[0] * group_size
    scale_factor = float(samples_all) ** (-0.5)
    genes = expression.shape[1] // group_size
    if genes % 128 == 0 and next_packed.shape[0] % 8 == 0:
        tiles, current_all, next_block = exchange(
            expression, current, next_packed, covariates, group_size
        )
        regrouped = tiles.reshape(samples_all, genes)
        everyone = current_all.reshape(samples_all, current.shape[1])
        return (over_samples(regrouped, everyone) * scale_factor, next_block)
    return shards_by_xla(expression, current, next_packed, covariates)


def shards_by_xla(expression, current, next_packed, covariates):
    group_size = lax.axis_size("samp")
    samples_all = expression.shape[0] * group_size
    scale_factor = float(samples_all) ** (-0.5)
    regrouped = lax.all_to_all(expression, "samp", split_axis=1, concat_axis=0, tiled=True)
    scores = (
        over_samples(regrouped, lax.all_gather(current, "samp", axis=0, tiled=True)) * scale_factor
    )
    packed_words = lax.all_to_all(next_packed, "samp", split_axis=1, concat_axis=0, tiled=True)
    dosage = unpack_words(packed_words)
    local_totals = jnp.sum(dosage, axis=0)
    local_proj = precise_samples(covariates, dosage)
    local_covsum = jnp.sum(covariates, axis=0)
    local_squares = jnp.sum(dosage * dosage, axis=0)
    local_gram = precise_samples(covariates, covariates)
    totals, projected, cov_sums, squares, cov_gram = lax.psum(
        (local_totals, local_proj, local_covsum, local_squares, local_gram), "samp"
    )
    average = totals / samples_all
    loading = projected - cov_sums[:, None] * average[None, :]
    leftover = (
        dosage - average[None, :] - jnp.dot(covariates, loading, precision=lax.Precision.HIGHEST)
    )
    mapped = jnp.dot(cov_gram, loading, precision=lax.Precision.HIGHEST)
    sq_norm = (
        squares
        - samples_all * average * average
        - 2.0 * jnp.sum(loading * loading, axis=0)
        + jnp.sum(loading * mapped, axis=0)
    )
    next_block = (leftover * lax.rsqrt(sq_norm / samples_all + 1e-05)[None, :]).astype(jnp.bfloat16)
    return (scores, next_block)


def solution(mesh):
    in_specs = (
        P(("parts", "samp"), None),
        P(("parts", "samp"), None),
        P(("parts", "samp"), None),
        P(("parts", "samp"), None),
    )
    out_specs = (P(("parts", "samp"), None), P(("parts", "samp"), None))
    return jax.shard_map(shards, mesh=mesh, in_specs=in_specs, out_specs=out_specs, check_vma=False)
```

```python
import functools

import jax
import jax.numpy as jnp
from jax import lax
from jax.experimental import pallas as pl
from jax.experimental.pallas import tpu as pltpu
from jax.sharding import PartitionSpec as P

MESH = pl.DeviceIdType.MESH
CORES = 2


def unpack_words(packed_words):
    shifts = 2 * jnp.arange(16, dtype=jnp.int32)
    fields = jnp.bitwise_and(
        lax.shift_right_logical(packed_words[:, :, None], shifts[None, None, :]), 3
    )
    return fields.reshape(packed_words.shape[0], -1).T.astype(jnp.float32)


def over_samples(left, right):
    return lax.dot_general(
        left, right, (((0,), (0,)), ((), ())), preferred_element_type=jnp.float32
    )


def precise_samples(left, right):
    return lax.dot_general(left, right, (((0,), (0,)), ((), ())), precision=lax.Precision.HIGHEST)


def grid_of(group_size):
    chips = group_size // CORES
    across = 2 ** ((chips.bit_length() - 1) // 3)
    return chips // across, across


def exchange_kernel(
    depth,
    across,
    genes,
    expr_ref,
    current_ref,
    packed_ref,
    cov_ref,
    tiles_ref,
    current_all,
    next_ref,
    cov_all,
    packed_all,
    dosage_ref,
    words_ref,
    own_sem,
    bulk_send,
    bulk_recv,
    small_send,
    small_recv,
    row_send,
    row_recv,
    ready_sem,
):
    me = lax.axis_index("samp")
    core = lax.rem(me, CORES)
    column = lax.rem(me // CORES, across)
    level = me // (CORES * across)
    group_size = CORES * across * depth
    rows = cov_ref.shape[0]
    last = depth - 1

    def at(z, x, c):
        return (z * across + x) * CORES + c

    def on_line(dz, act):
        z = level + dz
        pl.when(jnp.logical_and(z >= 0, z <= last))(functools.partial(act, z))

    row_mates = [
        (dx, dc) for dx in range(across) for dc in range(CORES) if (dx, dc) != (0, 0)
    ]

    def row_mate(z, dx, dc):
        return at(z, lax.rem(column + dx, across), lax.rem(core + dc, CORES))

    near_count = len(row_mates) + CORES * (
        jnp.where(level > 0, 1, 0) + jnp.where(level < last, 1, 0)
    )

    def greet(sem):
        def tell(target):
            pl.semaphore_signal(sem, inc=1, device_id={"samp": target}, device_id_type=MESH)

        def both_cores(z):
            for dc in range(CORES):
                tell(row_mate(z, 0, dc))

        on_line(1, both_cores)
        on_line(-1, both_cores)
        for dx, dc in row_mates:
            tell(row_mate(level, dx, dc))

    small = ((current_ref, current_all), (packed_ref, packed_all), (cov_ref, cov_all))

    def small_on_line(k, hop, step, source):
        own, whole = small[k]
        return pltpu.make_async_remote_copy(
            src_ref=own if hop == 0 else whole.at[source, column, core],
            dst_ref=whole.at[source, column, core],
            send_sem=small_send.at[k, hop * 2 + (step + 1) // 2],
            recv_sem=small_recv.at[k, source],
            device_id={"samp": at(level + step, column, core)},
            device_id_type=MESH,
        )

    def relay(hop, step, finish):
        source = level - hop * step
        goes = jnp.logical_and(
            jnp.logical_and(source >= 0, source <= last),
            jnp.logical_and(level + step >= 0, level + step <= last),
        )

        @pl.when(goes)
        def _():
            for k in range(len(small)):
                copy = small_on_line(k, hop, step, source)
                if finish:
                    copy.wait_send()
                else:
                    copy.start()

    def arrive(distance):
        def take(z):
            for k in range(len(small)):
                small_on_line(k, 1, 1, z).wait_recv()

        on_line(distance, take)
        on_line(-distance, take)

    def small_on_row(k, dx, sender_column):
        whole = small[k][1]
        return pltpu.make_async_remote_copy(
            src_ref=whole.at[:, column, core],
            dst_ref=whole.at[:, sender_column, core],
            send_sem=row_send.at[k, dx],
            recv_sem=row_recv.at[k, dx],
            device_id={"samp": at(level, lax.rem(column + dx, across), core)},
            device_id_type=MESH,
        )

    def small_to_core(k, sender_core):
        whole = small[k][1]
        return pltpu.make_async_remote_copy(
            src_ref=whole.at[:, :, core],
            dst_ref=whole.at[:, :, sender_core],
            send_sem=row_send.at[k, 0],
            recv_sem=row_recv.at[k, 0],
            device_id={"samp": at(level, column, 1 - core)},
            device_id_type=MESH,
        )

    def bulk(other, sender):
        span = pl.ds(pl.multiple_of(other * genes, 128), genes)
        return pltpu.make_async_remote_copy(
            src_ref=expr_ref.at[:, span],
            dst_ref=tiles_ref.at[sender],
            send_sem=bulk_send.at[other],
            recv_sem=bulk_recv.at[sender],
            device_id={"samp": other},
            device_id_type=MESH,
        )

    def send_tiles(dz, columns):
        def start(z):
            for dx in columns:
                for dc in range(CORES):
                    bulk(row_mate(z, dx, dc), me).start()

        on_line(dz, start)
        on_line(-dz, start)

    barrier = pltpu.get_barrier_semaphore()
    greet(barrier)
    own_copies = []
    for k, (own, whole) in enumerate(small):
        own_copies.append(
            pltpu.make_async_copy(own, whole.at[level, column, core], own_sem.at[k])
        )
    mine = pl.ds(pl.multiple_of(me * genes, 128), genes)
    own_copies.append(
        pltpu.make_async_copy(expr_ref.at[:, mine], tiles_ref.at[me], own_sem.at[len(small)])
    )
    for copy in own_copies:
        copy.start()
    pl.semaphore_wait(barrier, near_count)

    elsewhere = list(range(1, across))
    for hops in range(1, depth + 1):
        if hops < depth:
            greet(ready_sem.at[hops - 1])
        if hops == 1:
            relay(0, 1, False)
            relay(0, -1, False)
        if hops == 2:
            arrive(1)
            relay(1, 1, False)
            relay(1, -1, False)
        if hops < depth:
            send_tiles(hops, [0])
        if hops >= 2:
            send_tiles(hops - 1, elsewhere)
        if hops < depth:
            pl.semaphore_wait(ready_sem.at[hops - 1], near_count)
    for dx, dc in row_mates:
        bulk(row_mate(level, dx, dc), me).start()
    for distance in range(2, depth):
        arrive(distance)
        if distance < last:
            relay(distance, 1, False)
            relay(distance, -1, False)
    for copy in own_copies[: len(small)]:
        copy.wait()
    for dx in elsewhere:
        for k in range(len(small)):
            small_on_row(k, dx, column).start()
    for dx in elsewhere:
        for k in range(len(small)):
            small_on_row(k, dx, lax.rem(column - dx + across, across)).wait_recv()
    for k in range(len(small)):
        small_to_core(k, core).start()
    for k in range(len(small)):
        small_to_core(k, 1 - core).wait_recv()

    samples = group_size * rows
    variants = group_size * packed_ref.shape[0]
    word_count = packed_ref.shape[1]
    words_ref[...] = packed_all[...].reshape(variants, word_count).T
    shifts = 2 * lax.broadcasted_iota(jnp.int32, (16, variants), 0)

    @pl.loop(0, word_count)
    def _(word):
        held = jnp.broadcast_to(words_ref[pl.ds(word, 1), :], (16, variants))
        fields = jnp.bitwise_and(lax.shift_right_logical(held, shifts), 3)
        dosage_ref[pl.ds(pl.multiple_of(word * 16, 16), 16), :] = fields.astype(jnp.float32)

    cov = cov_all[...].reshape(samples, cov_ref.shape[1])
    average = jnp.sum(dosage_ref[...], axis=0, keepdims=True) / samples
    projected = precise_samples(cov, dosage_ref[...])
    cov_sums = precise_samples(cov, jnp.ones((samples, 128), jnp.float32))[:, :1]
    loading = projected - cov_sums * average
    leftover = (
        dosage_ref[...]
        - average
        - jnp.dot(cov, loading, precision=lax.Precision.HIGHEST, preferred_element_type=jnp.float32)
    )
    sq_norm = jnp.sum(leftover * leftover, axis=0, keepdims=True)
    dosage_ref[...] = leftover
    here = dosage_ref[pl.ds(pl.multiple_of(me * rows, 8), rows), :]
    next_ref[...] = (here * lax.rsqrt(sq_norm / samples + 1e-05)).astype(next_ref.dtype)

    own_copies[-1].wait()
    for step in range(1, group_size):
        bulk(lax.rem(me + step, group_size), me).wait_send()
    for step in range(1, group_size):
        bulk(me, lax.rem(me + step, group_size)).wait_recv()
    for hop in range(last):
        relay(hop, 1, True)
        relay(hop, -1, True)
    for k in range(len(small)):
        for dx in elsewhere:
            small_on_row(k, dx, column).wait_send()
        small_to_core(k, core).wait_send()


def exchange(expression, current, next_packed, covariates, group_size):
    depth, across = grid_of(group_size)
    rows, all_genes = expression.shape
    genes = all_genes // group_size
    variants = next_packed.shape[0] * group_size
    lead = (depth, across, CORES)
    vmem = pl.BlockSpec(memory_space=pltpu.VMEM)
    hbm = pl.BlockSpec(memory_space=pltpu.HBM)
    anywhere = pl.BlockSpec(memory_space=pl.ANY)
    return pl.pallas_call(
        functools.partial(exchange_kernel, depth, across, genes),
        out_shape=(
            jax.ShapeDtypeStruct((group_size, rows, genes), expression.dtype),
            jax.ShapeDtypeStruct((*lead, *current.shape), current.dtype),
            jax.ShapeDtypeStruct(current.shape, jnp.bfloat16),
        ),
        in_specs=[hbm] * 4,
        out_specs=(anywhere, vmem, vmem),
        scratch_shapes=[
            pltpu.VMEM((*lead, *covariates.shape), covariates.dtype),
            pltpu.VMEM((*lead, *next_packed.shape), next_packed.dtype),
            pltpu.VMEM((rows * group_size, variants), jnp.float32),
            pltpu.VMEM((next_packed.shape[1], variants), jnp.int32),
            pltpu.SemaphoreType.DMA((4,)),
            pltpu.SemaphoreType.DMA((group_size,)),
            pltpu.SemaphoreType.DMA((group_size,)),
            pltpu.SemaphoreType.DMA((3, 2 * depth)),
            pltpu.SemaphoreType.DMA((3, depth)),
            pltpu.SemaphoreType.DMA((3, across)),
            pltpu.SemaphoreType.DMA((3, across)),
            pltpu.SemaphoreType.REGULAR((depth,)),
        ],
        compiler_params=pltpu.CompilerParams(
            collective_id=0, has_side_effects=True
        ),
    )(expression, current, next_packed, covariates)


def scores_kernel(scale_factor, tiles_ref, current_ref, carried_ref, scores_ref, next_ref):
    scores_ref[...] = over_samples(tiles_ref[...], current_ref[...]) * scale_factor

    @pl.when(pl.program_id(0) == 0)
    def _():
        next_ref[...] = carried_ref[...]


def score(regrouped, everyone, next_block, scale_factor):
    samples, genes = regrouped.shape
    variants = everyone.shape[1]
    width = genes // 2 if genes % 256 == 0 else 128
    return pl.pallas_call(
        functools.partial(scores_kernel, scale_factor),
        grid=(genes // width,),
        out_shape=(
            jax.ShapeDtypeStruct((genes, variants), jnp.float32),
            jax.ShapeDtypeStruct(next_block.shape, next_block.dtype),
        ),
        in_specs=[
            pl.BlockSpec((samples, width), lambda i: (0, i)),
            pl.BlockSpec(everyone.shape, lambda i: (0, 0)),
            pl.BlockSpec(next_block.shape, lambda i: (0, 0)),
        ],
        out_specs=(
            pl.BlockSpec((width, variants), lambda i: (i, 0)),
            pl.BlockSpec(next_block.shape, lambda i: (0, 0)),
        ),
    )(regrouped, everyone, next_block)


def shards(expression, current, next_packed, covariates):
    group_size = lax.axis_size("samp")
    samples_all = expression.shape[0] * group_size
    scale_factor = float(samples_all) ** (-0.5)
    genes = expression.shape[1] // group_size
    if genes % 128 == 0 and next_packed.shape[0] % 8 == 0:
        tiles, current_all, next_block = exchange(
            expression, current, next_packed, covariates, group_size
        )
        regrouped = tiles.reshape(samples_all, genes)
        everyone = current_all.reshape(samples_all, current.shape[1])
        return tuple(score(regrouped, everyone, next_block, scale_factor))
    return shards_by_xla(expression, current, next_packed, covariates)


def shards_by_xla(expression, current, next_packed, covariates):
    group_size = lax.axis_size("samp")
    samples_all = expression.shape[0] * group_size
    scale_factor = float(samples_all) ** (-0.5)
    regrouped = lax.all_to_all(expression, "samp", split_axis=1, concat_axis=0, tiled=True)
    scores = (
        over_samples(regrouped, lax.all_gather(current, "samp", axis=0, tiled=True)) * scale_factor
    )
    packed_words = lax.all_to_all(next_packed, "samp", split_axis=1, concat_axis=0, tiled=True)
    dosage = unpack_words(packed_words)
    local_totals = jnp.sum(dosage, axis=0)
    local_proj = precise_samples(covariates, dosage)
    local_covsum = jnp.sum(covariates, axis=0)
    local_squares = jnp.sum(dosage * dosage, axis=0)
    local_gram = precise_samples(covariates, covariates)
    totals, projected, cov_sums, squares, cov_gram = lax.psum(
        (local_totals, local_proj, local_covsum, local_squares, local_gram), "samp"
    )
    average = totals / samples_all
    loading = projected - cov_sums[:, None] * average[None, :]
    leftover = (
        dosage - average[None, :] - jnp.dot(covariates, loading, precision=lax.Precision.HIGHEST)
    )
    mapped = jnp.dot(cov_gram, loading, precision=lax.Precision.HIGHEST)
    sq_norm = (
        squares
        - samples_all * average * average
        - 2.0 * jnp.sum(loading * loading, axis=0)
        + jnp.sum(loading * mapped, axis=0)
    )
    next_block = (leftover * lax.rsqrt(sq_norm / samples_all + 1e-05)[None, :]).astype(jnp.bfloat16)
    return (scores, next_block)


def solution(mesh):
    in_specs = (
        P(("parts", "samp"), None),
        P(("parts", "samp"), None),
        P(("parts", "samp"), None),
        P(("parts", "samp"), None),
    )
    out_specs = (P(("parts", "samp"), None), P(("parts", "samp"), None))
    return jax.shard_map(shards, mesh=mesh, in_specs=in_specs, out_specs=out_specs, check_vma=False)
```
